8 devices in a mesh: by: 2 (over z, y), bx: 4 (over x, core).
Axes of the slice: x: 2, y: 2, z: 1, core: 2. Of those that a mesh axis runs over, the one named last changes fastest.
Arguments:
- wave_fn: float32 [2048, 2, 2, 2048], P('bx', None, None, 'by')
- left_env: float32 [2048, 5, 2048], P('bx')
- mpo_ten: float32 [5, 2, 2, 5], replicated
- right_env: float32 [2048, 5, 2048], P('by')
Outputs:
- output: float32 [2048, 2, 2, 2048], P('bx', None, None, 'by')
All inputs are finite; a program needn't handle non-finite values.
Results may differ from the reference program's by a relative error of at most 0.001.
Values sent between devices are 32-bit elements.
A program may use at most 1 GiB of HBM per device.

```python
import jax
import jax.numpy as jnp
from jax import lax

BOND_DIM = 2048
PHYS_DIM = 2
MPO_DIM = 5


def setup_inputs(seed: int = 0) -> dict:
    key = jax.random.key(seed)
    k_wave, k_left, k_mpo, k_right = jax.random.split(key, 4)
    wave_fn = jax.random.normal(k_wave, (BOND_DIM, PHYS_DIM, PHYS_DIM, BOND_DIM), jnp.float32)
    left_env = jax.random.normal(k_left, (BOND_DIM, MPO_DIM, BOND_DIM), jnp.float32) * (BOND_DIM ** -0.5)
    mpo_ten = jax.random.normal(k_mpo, (MPO_DIM, PHYS_DIM, PHYS_DIM, MPO_DIM), jnp.float32) * ((MPO_DIM * PHYS_DIM) ** -0.5)
    right_env = jax.random.normal(k_right, (BOND_DIM, MPO_DIM, BOND_DIM), jnp.float32) * ((MPO_DIM * BOND_DIM) ** -0.5)
    return {'wave_fn': wave_fn, 'left_env': left_env, 'mpo_ten': mpo_ten, 'right_env': right_env}


def reference(wave_fn, left_env, mpo_ten, right_env):
    row_block = min(BOND_DIM, 128)
    block_count = BOND_DIM // row_block
    left_blocks = left_env.reshape(block_count, row_block, MPO_DIM, BOND_DIM)

    def one_block(left_rows):
        stage_one = jnp.einsum('auc,cpqf->aupqf', left_rows.astype(jnp.float32), wave_fn.astype(jnp.float32))
        stage_two = jnp.einsum('aupqf,uspv->asvqf', stage_one, mpo_ten.astype(jnp.float32))
        stage_three = jnp.einsum('asvqf,vtqr->astrf', stage_two, mpo_ten.astype(jnp.float32))
        return jnp.einsum('astrf,brf->astb', stage_three, right_env.astype(jnp.float32))

    out_blocks = lax.map(one_block, left_blocks)
    return out_blocks.reshape(BOND_DIM, PHYS_DIM, PHYS_DIM, BOND_DIM)
```

```python
import jax
import jax.numpy as jnp
from jax import lax
from jax.experimental import pallas as pl
from jax.experimental.pallas import tpu as pltpu
from jax.sharding import PartitionSpec as P

HI = lax.Precision.HIGHEST
F32 = jnp.float32
VMEM_LIMIT = 63 * 2**20
MESH = pl.DeviceIdType.MESH
ANY = pl.BlockSpec(memory_space=pl.ANY)


def greet(others):
    barrier = pltpu.get_barrier_semaphore()
    for other in others:
        pl.semaphore_signal(barrier, inc=1, device_id=other, device_id_type=MESH)
    pl.semaphore_wait(barrier, len(others))


def left_kernel(mix_hbm, left, xs, right, t3, t1, xg, rfar, buf, mix, mix_sem, send, recv):
    ta, tf, kb = 128, 256, 512
    by = lax.axis_index("by")
    bx = lax.axis_index("bx")
    core = lax.rem(bx, 2)
    chip = bx - core
    pair_bx = chip + 1 - core
    far_bx = lax.rem(bx + 2, 4)
    farpair_bx = lax.rem(pair_bx + 2, 4)
    pair = (by, pair_bx)
    far = (by, far_bx)
    across = (1 - by, bx)
    greet((pair, far, across))

    def remote(k, src, dst, to):
        return pltpu.make_async_remote_copy(
            src_ref=src, dst_ref=dst, send_sem=send.at[k], recv_sem=recv.at[k], device_id=to, device_id_type=MESH
        )

    to_pair = [remote(h, xs.at[h], xg.at[0, h], pair) for h in range(2)]
    to_far = [remote(2 + h, xs.at[h], xg.at[1, h], far) for h in range(2)]
    on_pair = [remote(4 + h, xg.at[1, h], xg.at[2, h], pair) for h in range(2)]
    rows = pl.ds(pl.multiple_of(core * 512, 512), 512)
    f_far = pl.ds(pl.multiple_of((1 - by) * 1024, 1024), 1024)
    r_across = remote(6, right.at[:, rows, f_far], rfar.at[:, rows, :], across)
    r_pair = remote(7, rfar.at[:, rows, :], rfar.at[:, rows, :], pair)

    to_pair[0].start()
    to_far[0].start()
    r_across.start()
    to_pair[1].start()
    to_far[1].start()
    get_mix = pltpu.make_async_copy(mix_hbm, mix, mix_sem)
    get_mix.start()
    get_mix.wait()

    def product(l0, l1, x0, x1):
        lhs = jnp.concatenate([l0[...].reshape(5 * ta, kb), l1[...].reshape(5 * ta, kb)], axis=1)
        rhs = jnp.concatenate([jnp.concatenate([x[i] for i in range(4)], axis=1) for x in (x0, x1)], axis=0)
        return jnp.dot(lhs, rhs, precision=HI, preferred_element_type=F32)

    def left_spec(col):
        return pl.BlockSpec((5, ta, kb), lambda j, i: (0, i, col))

    x_spec = pl.BlockSpec((4, kb, tf), lambda j, i: (0, 0, j))

    def t_spec(h):
        return pl.BlockSpec((5, 4, ta, tf), lambda j, i: (0, 0, i, 2 * h + j))

    def at_step(n, act):
        if act is not None:
            pl.when(pl.program_id(0) * 4 + pl.program_id(1) == n)(act)

    def first_half(h, n=0, act=None):
        def body(l0, l1, x0, x1, o):
            at_step(n, act)
            d = product(l0, l1, x0, x1)
            for u in range(5):
                for i in range(4):
                    o[u, i] = d[u * ta : (u + 1) * ta, i * tf : (i + 1) * tf]

        pltpu.emit_pipeline(
            body, grid=(2, 4), in_specs=[left_spec(bx), left_spec(pair_bx), x_spec, x_spec], out_specs=[t_spec(h)]
        )(left, left, xs.at[h], xg.at[0, h], t1)

    def second_half(h, n=0, act=None):
        def body(l0, l1, x0, x1, t, o):
            at_step(n, act)
            d = product(l0, l1, x0, x1)
            for u in range(5):
                for i in range(4):
                    buf[u, i] = d[u * ta : (u + 1) * ta, i * tf : (i + 1) * tf] + t[u, i]
            for a0 in range(0, ta, 16):
                m = jnp.concatenate(
                    [
                        jnp.concatenate([buf[u, i, a0 : a0 + 8], buf[u, i, a0 + 8 : a0 + 16]], axis=1)
                        for u in range(5)
                        for i in range(4)
                    ],
                    axis=0,
                )
                z = jnp.dot(mix[...], m, precision=HI, preferred_element_type=F32)
                for r in range(5):
                    for i in range(4):
                        row = (r * 4 + i) * 8
                        o[r, i, a0 : a0 + 8] = z[row : row + 8, :tf]
                        o[r, i, a0 + 8 : a0 + 16] = z[row : row + 8, tf:]

        pltpu.emit_pipeline(
            body,
            grid=(2, 4),
            in_specs=[left_spec(far_bx), left_spec(farpair_bx), x_spec, x_spec, t_spec(h)],
            out_specs=[t_spec(h)],
        )(left, left, xg.at[1, h], xg.at[2, h], t1, t3)

    def hand_on(k):
        def act():
            to_far[k].wait_recv()
            on_pair[k].start()

        return act

    def hand_on_right():
        r_across.wait_recv()
        r_pair.start()

    to_pair[0].wait_recv()
    first_half(0)
    to_pair[1].wait_recv()
    first_half(1, 5, hand_on(0))
    on_pair[0].wait_recv()
    second_half(0, 5, hand_on(1))
    on_pair[1].wait_recv()
    second_half(1, 3, hand_on_right)
    r_pair.wait_recv()
    for c in (*to_pair, *to_far, *on_pair, r_across, r_pair):
        c.wait_send()


def right_kernel(t3, rfar, right, y, held, got, send, recv):
    ta, tb = 128, 512
    by = lax.axis_index("by")
    bx = lax.axis_index("bx")
    across = (1 - by, bx)
    greet((across,))
    slots = held.shape[0]

    def remote(slot, tile):
        return pltpu.make_async_remote_copy(
            src_ref=held.at[slot],
            dst_ref=got.at[tile],
            send_sem=send.at[slot],
            recv_sem=recv.at[tile],
            device_id=across,
            device_id_type=MESH,
        )

    def product(t, b):
        lhs = jnp.concatenate([t[r].reshape(4 * ta, 1024) for r in range(5)], axis=1)
        rhs = jnp.concatenate([b[r] for r in range(5)], axis=1)
        d = lax.dot_general(lhs, rhs, (((1,), (1,)), ((), ())), precision=HI, preferred_element_type=F32)
        return d.reshape(4, ta, tb)

    t_spec = pl.BlockSpec((5, 4, ta, 1024), lambda j, i: (0, 0, i, 0))

    def far_body(t, b):
        tile = pl.program_id(0) * 4 + pl.program_id(1)
        slot = lax.rem(tile, slots)

        @pl.when(tile >= slots)
        def _():
            remote(slot, tile).wait_send()

        held[slot] = product(t, b)
        remote(slot, tile).start()

    pltpu.emit_pipeline(
        far_body,
        grid=(2, 4),
        in_specs=[t_spec, pl.BlockSpec((5, tb, 1024), lambda j, i: (0, j, 0))],
        out_specs=[],
    )(t3, rfar)

    def own_body(t, b, o):
        tile = pl.program_id(0) * 4 + pl.program_id(1)
        d = product(t, b)
        remote(0, tile).wait_recv()
        o[...] = d + got[tile]

    pltpu.emit_pipeline(
        own_body,
        grid=(2, 4),
        in_specs=[t_spec, pl.BlockSpec((5, tb, 1024), lambda j, i: (0, j, by))],
        out_specs=[pl.BlockSpec((4, ta, tb), lambda j, i: (0, i, j))],
    )(t3, right, y)
    for slot in range(slots):
        remote(slot, 0).wait_send()


def order_kernel(w, o):
    for p in range(2):
        for q in range(2):
            for j in range(8):
                o[j // 4, p * 2 + q, :, (j % 4) * 128 : (j % 4 + 1) * 128] = w[
                    pl.ds(p * 16 + j * 2 + q, o.shape[2], stride=32), :
                ]


def solution(mesh):
    def local_apply(wave_blk, left_rows, mpo_ten, right_rows):
        left = jnp.transpose(left_rows, (1, 0, 2))
        right = jnp.transpose(right_rows, (1, 0, 2))
        wave = jnp.transpose(wave_blk.reshape(512, 2, 2, 8, 128), (0, 1, 3, 2, 4)).reshape(512 * 32, 128)
        xs = pl.pallas_call(
            order_kernel,
            grid=(8,),
            in_specs=[pl.BlockSpec((64 * 32, 128), lambda i: (i, 0))],
            out_specs=pl.BlockSpec((2, 4, 64, 512), lambda i: (0, 0, i, 0)),
            out_shape=jax.ShapeDtypeStruct((2, 4, 512, 512), F32),
            name="order",
        )(wave)
        w2 = jnp.einsum("uspv,vtqr->rstupq", mpo_ten, mpo_ten, precision=HI, preferred_element_type=F32)
        mix = (w2.reshape(20, 1, 20, 1) * jnp.eye(8, dtype=F32).reshape(1, 8, 1, 8)).reshape(160, 160)

        t3, _, _, rfar = pl.pallas_call(
            left_kernel,
            in_specs=[ANY] * 4,
            out_specs=[ANY] * 4,
            out_shape=[
                jax.ShapeDtypeStruct((5, 4, 512, 1024), F32),
                jax.ShapeDtypeStruct((5, 4, 512, 1024), F32),
                jax.ShapeDtypeStruct((3, 2, 4, 512, 512), F32),
                jax.ShapeDtypeStruct((5, 1024, 1024), F32),
            ],
            scratch_shapes=[
                pltpu.VMEM((5, 4, 128, 256), F32),
                pltpu.VMEM((160, 160), F32),
                pltpu.SemaphoreType.DMA,
                pltpu.SemaphoreType.DMA((8,)),
                pltpu.SemaphoreType.DMA((8,)),
            ],
            compiler_params=pltpu.CompilerParams(
                collective_id=0, has_side_effects=True, vmem_limit_bytes=VMEM_LIMIT
            ),
            name="left_part",
        )(mix, left, xs, right)

        y = pl.pallas_call(
            right_kernel,
            in_specs=[ANY] * 3,
            out_specs=ANY,
            out_shape=jax.ShapeDtypeStruct((4, 512, 1024), F32),
            scratch_shapes=[
                pltpu.VMEM((4, 4, 128, 512), F32),
                pltpu.VMEM((8, 4, 128, 512), F32),
                pltpu.SemaphoreType.DMA((4,)),
                pltpu.SemaphoreType.DMA((8,)),
            ],
            compiler_params=pltpu.CompilerParams(
                collective_id=1, has_side_effects=True, vmem_limit_bytes=VMEM_LIMIT
            ),
            name="right_part",
        )(t3, rfar, right)
        return jnp.transpose(y, (1, 0, 2)).reshape(512, 2, 2, 1024)

    return jax.shard_map(
        local_apply,
        mesh=mesh,
        in_specs=(P("bx", None, None, "by"), P("bx", None, None), P(), P("by", None, None)),
        out_specs=P("bx", None, None, "by"),
        check_vma=False,
    )
```

```python
import jax
import jax.numpy as jnp
from jax import lax
from jax.experimental import pallas as pl
from jax.experimental.pallas import tpu as pltpu
from jax.sharding import PartitionSpec as P

HI = lax.Precision.HIGHEST
F32 = jnp.float32
VMEM_LIMIT = 63 * 2**20
MESH = pl.DeviceIdType.MESH
ANY = pl.BlockSpec(memory_space=pl.ANY)


def greet(others):
    barrier = pltpu.get_barrier_semaphore()
    for other in others:
        pl.semaphore_signal(barrier, inc=1, device_id=other, device_id_type=MESH)
    pl.semaphore_wait(barrier, len(others))


def apply_kernel(
    mix_hbm, left, xs, right, y, t3, t1, xg, rfar, got, buf, mix, rbuf, held, gbuf, sem, rsem, send, recv, tsend, trecv
):
    ta, tf, kb, tb = 128, 256, 512, 512
    by = lax.axis_index("by")
    bx = lax.axis_index("bx")
    core = lax.rem(bx, 2)
    pair_bx = bx + 1 - 2 * core
    far_bx = lax.rem(bx + 2, 4)
    farpair_bx = lax.rem(pair_bx + 2, 4)
    pair = (by, pair_bx)
    far = (by, far_bx)
    across = (1 - by, bx)
    greet((pair, far, across))

    def remote(k, src, dst, to):
        return pltpu.make_async_remote_copy(
            src_ref=src, dst_ref=dst, send_sem=send.at[k], recv_sem=recv.at[k], device_id=to, device_id_type=MESH
        )

    def to_pair(k):
        cols = pl.ds(pl.multiple_of(k % 2 * tf, tf), tf)
        return remote(6 + k, xs.at[k // 2, :, :, cols], xg.at[0, k // 2, :, :, cols], pair)

    def to_far(h):
        return remote(h, xs.at[h], xg.at[1, h], far)

    def on_pair(h):
        return remote(2 + h, xg.at[1, h], xg.at[2, h], pair)

    rows = pl.ds(pl.multiple_of(core * 512, 512), 512)
    f_far = pl.ds(pl.multiple_of((1 - by) * 1024, 1024), 1024)
    f_own = pl.ds(pl.multiple_of(by * 1024, 1024), 1024)
    r_across = remote(4, right.at[:, rows, f_far], rfar.at[:, rows, :], across)
    r_pair = remote(5, rfar.at[:, rows, :], rfar.at[:, rows, :], pair)

    to_pair(0).start()
    to_far(0).start()
    r_across.start()
    for k in range(1, 4):
        to_pair(k).start()
    to_far(1).start()
    get_mix = pltpu.make_async_copy(mix_hbm, mix, sem.at[0])
    get_mix.start()
    to_pair(0).wait_recv()

    def right_far(n):
        src = rfar.at[:, pl.ds(pl.multiple_of(n * tb, tb), tb), :]
        return pltpu.make_async_copy(src, rbuf.at[n % 2], rsem.at[n % 2])

    def right_own(n):
        src = right.at[:, pl.ds(pl.multiple_of((n - 2) * tb, tb), tb), f_own]
        return pltpu.make_async_copy(src, rbuf.at[n % 2], rsem.at[n % 2])

    def product(l0, l1, x0, x1):
        lhs = jnp.concatenate([l0[...].reshape(5 * ta, kb), l1[...].reshape(5 * ta, kb)], axis=1)
        rhs = jnp.concatenate([jnp.concatenate([x[i] for i in range(4)], axis=1) for x in (x0, x1)], axis=0)
        return jnp.dot(lhs, rhs, precision=HI, preferred_element_type=F32)

    def left_spec(col):
        return pl.BlockSpec((5, ta, kb), lambda j, i: (0, i, col))

    x_spec = pl.BlockSpec((4, kb, tf), lambda j, i: (0, 0, j))

    def first_half(h, _):
        def body(l0, l1, x0, x1, o):
            step = pl.program_id(0) * 4 + pl.program_id(1)

            for k in range(1, 4):

                @pl.when(step + 8 * h == (1, 3, 6)[k - 1])
                def _(k=k):
                    to_pair(k).wait_recv()

            @pl.when(step + 8 * h == 13)
            def _():
                to_far(0).wait_recv()
                on_pair(0).start()

            d = product(l0, l1, x0, x1)
            for u in range(5):
                for i in range(4):
                    o[u, i] = d[u * ta : (u + 1) * ta, i * tf : (i + 1) * tf]

        t_spec = pl.BlockSpec((5, 4, ta, tf), lambda j, i: (0, 0, i, 2 * h + j))
        pltpu.emit_pipeline(
            body, grid=(2, 4), in_specs=[left_spec(bx), left_spec(pair_bx), x_spec, x_spec], out_specs=[t_spec]
        )(left, left, xs.at[h], xg.at[0, h], t1)
        return 0

    lax.fori_loop(0, 2, first_half, 0)

    def second_half(h, _):
        on_pair(h).wait_recv()

        def body(l0, l1, x0, x1, t, o):
            step = pl.program_id(0) * 4 + pl.program_id(1) + 8 * h

            @pl.when(step == 5)
            def _():
                to_far(1).wait_recv()
                on_pair(1).start()

            @pl.when(step == 11)
            def _():
                r_across.wait_recv()
                r_pair.start()

            @pl.when(step == 15)
            def _():
                r_pair.wait_recv()
                right_far(0).start()

            d = product(l0, l1, x0, x1)
            for u in range(5):
                for i in range(4):
                    buf[u, i] = d[u * ta : (u + 1) * ta, i * tf : (i + 1) * tf] + t[u, i]
            for a0 in range(0, ta, 16):
                m = jnp.concatenate(
                    [
                        jnp.concatenate([buf[u, i, a0 : a0 + 8], buf[u, i, a0 + 8 : a0 + 16]], axis=1)
                        for u in range(5)
                        for i in range(4)
                    ],
                    axis=0,
                )
                z = jnp.dot(mix[...], m, precision=HI, preferred_element_type=F32)
                for r in range(5):
                    for i in range(4):
                        row = (r * 4 + i) * 8
                        o[r, i, a0 : a0 + 8] = z[row : row + 8, :tf]
                        o[r, i, a0 + 8 : a0 + 16] = z[row : row + 8, tf:]

        t_spec = pl.BlockSpec((5, 4, ta, tf), lambda j, i: (0, 0, i, 2 * h + j))
        pltpu.emit_pipeline(
            body,
            grid=(2, 4),
            in_specs=[left_spec(far_bx), left_spec(farpair_bx), x_spec, x_spec, t_spec],
            out_specs=[t_spec],
        )(left, left, xg.at[1, h], xg.at[2, h], t1, t3)
        return 0

    get_mix.wait()
    lax.fori_loop(0, 2, second_half, 0)

    def tile_copy(tile):
        slot = lax.rem(tile, 4)
        return pltpu.make_async_remote_copy(
            src_ref=held.at[slot],
            dst_ref=got.at[tile],
            send_sem=tsend.at[slot],
            recv_sem=trecv.at[tile],
            device_id=across,
            device_id_type=MESH,
        )

    def right_body(t, o):
        n = pl.program_id(0)
        i = pl.program_id(1)
        tile = n * 4 + i
        slot = lax.rem(tile, 4)

        def block(k, act):
            @pl.when(jnp.logical_and(i == 0, n == k))
            def _():
                act()

        for k in range(4):

            def act(k=k):
                (right_far(k) if k < 2 else right_own(k)).wait()
                if k < 3:
                    (right_far(k + 1) if k + 1 < 2 else right_own(k + 1)).start()

            block(k, act)

        arrived = pltpu.make_async_copy(got.at[jnp.maximum(tile - 8, 0)], gbuf, sem.at[1])

        @pl.when(jnp.logical_and(tile >= 4, n < 2))
        def _():
            tile_copy(tile - 4).wait_send()

        @pl.when(n >= 2)
        def _():
            tile_copy(tile - 8).wait_recv()
            arrived.start()

        lhs = jnp.concatenate([t[r].reshape(4 * ta, 1024) for r in range(5)], axis=1)
        half = lax.rem(n, 2)
        rhs = jnp.concatenate([rbuf[half, r] for r in range(5)], axis=1)
        d = lax.dot_general(lhs, rhs, (((1,), (1,)), ((), ())), precision=HI, preferred_element_type=F32)
        o[...] = d.reshape(4, ta, tb)

        @pl.when(n < 2)
        def _():
            held[slot] = o[...]
            tile_copy(tile).start()

        @pl.when(n >= 2)
        def _():
            arrived.wait()
            o[...] += gbuf[...]

    pltpu.emit_pipeline(
        right_body,
        grid=(4, 4),
        in_specs=[pl.BlockSpec((5, 4, ta, 1024), lambda n, i: (0, 0, i, 0))],
        out_specs=[pl.BlockSpec((4, ta, tb), lambda n, i: (0, (n // 2) * i, (n // 2) * (n - 2)))],
    )(t3, y)
    for tile in range(4, 8):
        tile_copy(tile).wait_send()
    for k in range(4):
        to_pair(k).wait_send()
    for h in range(2):
        to_far(h).wait_send()
        on_pair(h).wait_send()
    r_across.wait_send()
    r_pair.wait_send()


PITCH = 40


def order_kernel(w, o, raw, sem):
    step = pl.program_id(0)
    cs = raw.shape[1]

    def fetch(k):
        return pltpu.make_async_copy(
            w.at[pl.ds(k * cs, cs)], raw.at[lax.rem(k, 2), :, 0:32, :], sem.at[lax.rem(k, 2)]
        )

    @pl.when(step == 0)
    def _():
        fetch(0).start()

    @pl.when(step + 1 < pl.num_programs(0))
    def _():
        fetch(step + 1).start()

    fetch(step).wait()
    flat = raw.at[lax.rem(step, 2)].reshape(cs * PITCH, 128)
    for p in range(2):
        for q in range(2):
            for j in range(8):
                o[j // 4, p * 2 + q, :, (j % 4) * 128 : (j % 4 + 1) * 128] = flat[
                    pl.ds(p * 16 + j * 2 + q, cs, stride=PITCH), :
                ]


def place_kernel(y, o, raw, sem):
    step = pl.program_id(0)
    cs = raw.shape[1]

    def store(k):
        return pltpu.make_async_copy(
            raw.at[lax.rem(k, 2), :, 0:32, :], o.at[pl.ds(k * cs, cs)], sem.at[lax.rem(k, 2)]
        )

    @pl.when(step >= 2)
    def _():
        store(step - 2).wait()

    flat = raw.at[lax.rem(step, 2)].reshape(cs * PITCH, 128)
    for s in range(2):
        for t in range(2):
            for j in range(8):
                flat[pl.ds(s * 16 + j * 2 + t, cs, stride=PITCH), :] = y[s * 2 + t, :, j * 128 : (j + 1) * 128]
    store(step).start()

    @pl.when(step + 1 == pl.num_programs(0))
    def _():
        store(step - 1).wait()
        store(step).wait()


def solution(mesh):
    def local_apply(wave_blk, left_rows, mpo_ten, right_rows):
        left = jnp.transpose(left_rows, (1, 0, 2))
        right = jnp.transpose(right_rows, (1, 0, 2))
        wave = jnp.transpose(wave_blk.reshape(512, 2, 2, 8, 128), (0, 1, 3, 2, 4)).reshape(512, 32, 128)
        cs = 128
        edge = [pltpu.VMEM((2, cs, PITCH, 128), F32), pltpu.SemaphoreType.DMA((2,))]
        xs = pl.pallas_call(
            order_kernel,
            grid=(512 // cs,),
            in_specs=[ANY],
            out_specs=pl.BlockSpec((2, 4, cs, 512), lambda i: (0, 0, i, 0)),
            out_shape=jax.ShapeDtypeStruct((2, 4, 512, 512), F32),
            scratch_shapes=edge,
            name="order",
        )(wave)
        w2 = jnp.einsum("uspv,vtqr->rstupq", mpo_ten, mpo_ten, precision=HI, preferred_element_type=F32)
        mix = (w2.reshape(20, 1, 20, 1) * jnp.eye(8, dtype=F32).reshape(1, 8, 1, 8)).reshape(160, 160)

        y = pl.pallas_call(
            apply_kernel,
            in_specs=[ANY] * 4,
            out_specs=[ANY] * 6,
            out_shape=[
                jax.ShapeDtypeStruct((4, 512, 1024), F32),
                jax.ShapeDtypeStruct((5, 4, 512, 1024), F32),
                jax.ShapeDtypeStruct((5, 4, 512, 1024), F32),
                jax.ShapeDtypeStruct((3, 2, 4, 512, 512), F32),
                jax.ShapeDtypeStruct((5, 1024, 1024), F32),
                jax.ShapeDtypeStruct((8, 4, 128, 512), F32),
            ],
            scratch_shapes=[
                pltpu.VMEM((5, 4, 128, 256), F32),
                pltpu.VMEM((160, 160), F32),
                pltpu.VMEM((2, 5, 512, 1024), F32),
                pltpu.VMEM((4, 4, 128, 512), F32),
                pltpu.VMEM((4, 128, 512), F32),
                pltpu.SemaphoreType.DMA((2,)),
                pltpu.SemaphoreType.DMA((2,)),
                pltpu.SemaphoreType.DMA((10,)),
                pltpu.SemaphoreType.DMA((10,)),
                pltpu.SemaphoreType.DMA((4,)),
                pltpu.SemaphoreType.DMA((8,)),
            ],
            compiler_params=pltpu.CompilerParams(
                collective_id=0, has_side_effects=True, vmem_limit_bytes=VMEM_LIMIT
            ),
            name="apply",
        )(mix, left, xs, right)[0]

        out = pl.pallas_call(
            place_kernel,
            grid=(512 // cs,),
            in_specs=[pl.BlockSpec((4, cs, 1024), lambda i: (0, i, 0))],
            out_specs=ANY,
            out_shape=jax.ShapeDtypeStruct((512, 32, 128), F32),
            scratch_shapes=edge,
            name="place",
        )(y)
        return jnp.transpose(out.reshape(512, 2, 8, 2, 128), (0, 1, 3, 2, 4)).reshape(512, 2, 2, 1024)

    return jax.shard_map(
        local_apply,
        mesh=mesh,
        in_specs=(P("bx", None, None, "by"), P("bx", None, None), P(), P("by", None, None)),
        out_specs=P("bx", None, None, "by"),
        check_vma=False,
    )
```

```python
import jax
import jax.numpy as jnp
from jax import lax
from jax.experimental import pallas as pl
from jax.experimental.pallas import tpu as pltpu
from jax.sharding import PartitionSpec as P

HI = lax.Precision.HIGHEST
F32 = jnp.float32
VMEM_LIMIT = 63 * 2**20
MESH = pl.DeviceIdType.MESH
ANY = pl.BlockSpec(memory_space=pl.ANY)


def greet(others):
    barrier = pltpu.get_barrier_semaphore()
    for other in others:
        pl.semaphore_signal(barrier, inc=1, device_id=other, device_id_type=MESH)
    pl.semaphore_wait(barrier, len(others))


def apply_kernel(
    mix_hbm, left, xs, right, y, t3, xg, rfar, got, tbuf, mix, rbuf, held, gbuf, sem, rsem, send, recv, tsend, trecv
):
    ta, tf, kb, tb = 128, 256, 512, 512
    by = lax.axis_index("by")
    bx = lax.axis_index("bx")
    core = lax.rem(bx, 2)
    pair_bx = bx + 1 - 2 * core
    far_bx = lax.rem(bx + 2, 4)
    farpair_bx = lax.rem(pair_bx + 2, 4)
    pair = (by, pair_bx)
    far = (by, far_bx)
    across = (1 - by, bx)
    greet((pair, far, across))

    def remote(k, src, dst, to):
        return pltpu.make_async_remote_copy(
            src_ref=src, dst_ref=dst, send_sem=send.at[k], recv_sem=recv.at[k], device_id=to, device_id_type=MESH
        )

    def to_pair(k):
        cols = pl.ds(pl.multiple_of(k % 2 * tf, tf), tf)
        return remote(6 + k, xg.at[0, k // 2, :, :, cols], xg.at[1, k // 2, :, :, cols], pair)

    def to_far(h):
        return remote(h, xg.at[0, h], xg.at[2, h], far)

    def on_pair(h):
        return remote(2 + h, xg.at[2, h], xg.at[3, h], pair)

    rows = pl.ds(pl.multiple_of(core * 512, 512), 512)
    f_far = pl.ds(pl.multiple_of((1 - by) * 1024, 1024), 1024)
    f_own = pl.ds(pl.multiple_of(by * 1024, 1024), 1024)
    r_across = remote(4, right.at[:, rows, f_far], rfar.at[:, rows, :], across)
    r_pair = remote(5, rfar.at[:, rows, :], rfar.at[:, rows, :], pair)

    to_pair(0).start()
    to_far(0).start()
    r_across.start()
    for k in range(1, 4):
        to_pair(k).start()
    to_far(1).start()
    get_mix = pltpu.make_async_copy(mix_hbm, mix, sem.at[0])
    get_mix.start()
    to_pair(0).wait_recv()

    def right_far(n):
        src = rfar.at[:, pl.ds(pl.multiple_of(n * tb, tb), tb), :]
        return pltpu.make_async_copy(src, rbuf.at[n % 2], rsem.at[n % 2])

    def right_own(n):
        src = right.at[:, pl.ds(pl.multiple_of((n - 2) * tb, tb), tb), f_own]
        return pltpu.make_async_copy(src, rbuf.at[n % 2], rsem.at[n % 2])

    x_spec = pl.BlockSpec((4, kb, tf), lambda j, i: (0, 0, j))

    def left_half(part, _):
        s = part // 2
        h = lax.rem(part, 2)
        col0 = (1 - s) * bx + s * far_bx
        col1 = (1 - s) * pair_bx + s * farpair_bx

        @pl.when(part == 2)
        def _():
            get_mix.wait()
            on_pair(0).wait_recv()

        @pl.when(part == 3)
        def _():
            on_pair(1).wait_recv()

        def body(l0, l1, x0, x1, o):
            j = pl.program_id(0)
            i = pl.program_id(1)
            step = part * 8 + j * 4 + i

            def at(n, act):
                @pl.when(step == n)
                def _():
                    act()

            def on_far(k):
                to_far(k).wait_recv()
                on_pair(k).start()

            def on_right():
                r_across.wait_recv()
                r_pair.start()

            def first_right():
                r_pair.wait_recv()
                right_far(0).start()

            at(1, to_pair(1).wait_recv)
            at(3, to_pair(2).wait_recv)
            at(6, to_pair(3).wait_recv)
            at(13, lambda: on_far(0))
            at(21, lambda: on_far(1))
            at(27, on_right)
            at(31, first_right)

            rows_i = pl.ds(pl.multiple_of(i * ta, ta), ta)
            cols_j = pl.ds(pl.multiple_of((2 * h + j) * tf, tf), tf)
            get_t = pltpu.make_async_copy(t3.at[:, :, rows_i, cols_j], tbuf, sem.at[1])

            @pl.when(s == 1)
            def _():
                get_t.start()

            lhs = jnp.concatenate([l0[...].reshape(5 * ta, kb), l1[...].reshape(5 * ta, kb)], axis=1)
            rhs = jnp.concatenate([jnp.concatenate([x[n] for n in range(4)], axis=1) for x in (x0, x1)], axis=0)
            d = jnp.dot(lhs, rhs, precision=HI, preferred_element_type=F32)
            for u in range(5):
                for n in range(4):
                    o[u, n] = d[u * ta : (u + 1) * ta, n * tf : (n + 1) * tf]

            @pl.when(s == 1)
            def _():
                get_t.wait()
                for a0 in range(0, ta, 16):
                    m = jnp.concatenate(
                        [
                            jnp.concatenate(
                                [o[u, n, b : b + 8] + tbuf[u, n, b : b + 8] for b in (a0, a0 + 8)], axis=1
                            )
                            for u in range(5)
                            for n in range(4)
                        ],
                        axis=0,
                    )
                    z = jnp.dot(mix[...], m, precision=HI, preferred_element_type=F32)
                    for r in range(5):
                        for n in range(4):
                            row = (r * 4 + n) * 8
                            o[r, n, a0 : a0 + 8] = z[row : row + 8, :tf]
                            o[r, n, a0 + 8 : a0 + 16] = z[row : row + 8, tf:]

        pltpu.emit_pipeline(
            body,
            grid=(2, 4),
            in_specs=[
                pl.BlockSpec((5, ta, kb), lambda j, i: (0, i, col0)),
                pl.BlockSpec((5, ta, kb), lambda j, i: (0, i, col1)),
                x_spec,
                x_spec,
            ],
            out_specs=[pl.BlockSpec((5, 4, ta, tf), lambda j, i: (0, 0, i, 2 * h + j))],
        )(left, left, xg.at[2 * s, h], xg.at[2 * s + 1, h], t3)
        return 0

    lax.fori_loop(0, 4, left_half, 0)

    def tile_copy(tile):
        slot = lax.rem(tile, 4)
        return pltpu.make_async_remote_copy(
            src_ref=held.at[slot],
            dst_ref=got.at[tile],
            send_sem=tsend.at[slot],
            recv_sem=trecv.at[tile],
            device_id=across,
            device_id_type=MESH,
        )

    def right_body(t, o):
        n = pl.program_id(0)
        i = pl.program_id(1)
        tile = n * 4 + i
        slot = lax.rem(tile, 4)

        def block(k, act):
            @pl.when(jnp.logical_and(i == 0, n == k))
            def _():
                act()

        for k in range(4):

            def act(k=k):
                (right_far(k) if k < 2 else right_own(k)).wait()
                if k < 3:
                    (right_far(k + 1) if k + 1 < 2 else right_own(k + 1)).start()

            block(k, act)

        arrived = pltpu.make_async_copy(got.at[jnp.maximum(tile - 8, 0)], gbuf, sem.at[1])

        @pl.when(jnp.logical_and(tile >= 4, n < 2))
        def _():
            tile_copy(tile - 4).wait_send()

        @pl.when(n >= 2)
        def _():
            tile_copy(tile - 8).wait_recv()
            arrived.start()

        lhs = jnp.concatenate([t[r].reshape(4 * ta, 1024) for r in range(5)], axis=1)
        half = lax.rem(n, 2)
        rhs = jnp.concatenate([rbuf[half, r] for r in range(5)], axis=1)
        d = lax.dot_general(lhs, rhs, (((1,), (1,)), ((), ())), precision=HI, preferred_element_type=F32)
        o[...] = d.reshape(4, ta, tb)

        @pl.when(n < 2)
        def _():
            held[slot] = o[...]
            tile_copy(tile).start()

        @pl.when(n >= 2)
        def _():
            arrived.wait()
            o[...] += gbuf[...]

    pltpu.emit_pipeline(
        right_body,
        grid=(4, 4),
        in_specs=[pl.BlockSpec((5, 4, ta, 1024), lambda n, i: (0, 0, i, 0))],
        out_specs=[pl.BlockSpec((4, ta, tb), lambda n, i: (0, (n // 2) * i, (n // 2) * (n - 2)))],
    )(t3, y)
    for tile in range(4, 8):
        tile_copy(tile).wait_send()
    for k in range(4):
        to_pair(k).wait_send()
    for h in range(2):
        to_far(h).wait_send()
        on_pair(h).wait_send()
    r_across.wait_send()
    r_pair.wait_send()


PITCH = 40


def order_kernel(w, o, raw, sem):
    step = pl.program_id(0)
    cs = raw.shape[1]

    def fetch(k):
        return pltpu.make_async_copy(
            w.at[pl.ds(k * cs, cs)], raw.at[lax.rem(k, 2), :, 0:32, :], sem.at[lax.rem(k, 2)]
        )

    @pl.when(step == 0)
    def _():
        fetch(0).start()

    @pl.when(step + 1 < pl.num_programs(0))
    def _():
        fetch(step + 1).start()

    fetch(step).wait()
    flat = raw.at[lax.rem(step, 2)].reshape(cs * PITCH, 128)
    for p in range(2):
        for q in range(2):
            for j in range(8):
                o[0, j // 4, p * 2 + q, :, (j % 4) * 128 : (j % 4 + 1) * 128] = flat[
                    pl.ds(p * 16 + j * 2 + q, cs, stride=PITCH), :
                ]


def place_kernel(y, o, raw, sem):
    step = pl.program_id(0)
    cs = raw.shape[1]

    def store(k):
        return pltpu.make_async_copy(
            raw.at[lax.rem(k, 2), :, 0:32, :], o.at[pl.ds(k * cs, cs)], sem.at[lax.rem(k, 2)]
        )

    @pl.when(step >= 2)
    def _():
        store(step - 2).wait()

    flat = raw.at[lax.rem(step, 2)].reshape(cs * PITCH, 128)
    for s in range(2):
        for t in range(2):
            for j in range(8):
                flat[pl.ds(s * 16 + j * 2 + t, cs, stride=PITCH), :] = y[s * 2 + t, :, j * 128 : (j + 1) * 128]
    store(step).start()

    @pl.when(step + 1 == pl.num_programs(0))
    def _():
        store(step - 1).wait()
        store(step).wait()


def solution(mesh):
    def local_apply(wave_blk, left_rows, mpo_ten, right_rows):
        left = jnp.transpose(left_rows, (1, 0, 2))
        right = jnp.transpose(right_rows, (1, 0, 2))
        wave = jnp.transpose(wave_blk.reshape(512, 2, 2, 8, 128), (0, 1, 3, 2, 4)).reshape(512, 32, 128)
        cs = 128
        edge = [pltpu.VMEM((2, cs, PITCH, 128), F32), pltpu.SemaphoreType.DMA((2,))]
        xs = pl.pallas_call(
            order_kernel,
            grid=(512 // cs,),
            in_specs=[ANY],
            out_specs=pl.BlockSpec((1, 2, 4, cs, 512), lambda i: (0, 0, 0, i, 0)),
            out_shape=jax.ShapeDtypeStruct((4, 2, 4, 512, 512), F32),
            scratch_shapes=edge,
            name="order",
        )(wave)
        w2 = jnp.einsum("uspv,vtqr->rstupq", mpo_ten, mpo_ten, precision=HI, preferred_element_type=F32)
        mix = (w2.reshape(20, 1, 20, 1) * jnp.eye(8, dtype=F32).reshape(1, 8, 1, 8)).reshape(160, 160)

        y = pl.pallas_call(
            apply_kernel,
            in_specs=[ANY] * 4,
            out_specs=[ANY] * 5,
            out_shape=[
                jax.ShapeDtypeStruct((4, 512, 1024), F32),
                jax.ShapeDtypeStruct((5, 4, 512, 1024), F32),
                jax.ShapeDtypeStruct((4, 2, 4, 512, 512), F32),
                jax.ShapeDtypeStruct((5, 1024, 1024), F32),
                jax.ShapeDtypeStruct((8, 4, 128, 512), F32),
            ],
            input_output_aliases={2: 2},
            scratch_shapes=[
                pltpu.VMEM((5, 4, 128, 256), F32),
                pltpu.VMEM((160, 160), F32),
                pltpu.VMEM((2, 5, 512, 1024), F32),
                pltpu.VMEM((4, 4, 128, 512), F32),
                pltpu.VMEM((4, 128, 512), F32),
                pltpu.SemaphoreType.DMA((2,)),
                pltpu.SemaphoreType.DMA((2,)),
                pltpu.SemaphoreType.DMA((10,)),
                pltpu.SemaphoreType.DMA((10,)),
                pltpu.SemaphoreType.DMA((4,)),
                pltpu.SemaphoreType.DMA((8,)),
            ],
            compiler_params=pltpu.CompilerParams(
                collective_id=0, has_side_effects=True, vmem_limit_bytes=VMEM_LIMIT
            ),
            name="apply",
        )(mix, left, xs, right)[0]

        out = pl.pallas_call(
            place_kernel,
            grid=(512 // cs,),
            in_specs=[pl.BlockSpec((4, cs, 1024), lambda i: (0, i, 0))],
            out_specs=ANY,
            out_shape=jax.ShapeDtypeStruct((512, 32, 128), F32),
            scratch_shapes=edge,
            name="place",
        )(y)
        return jnp.transpose(out.reshape(512, 2, 8, 2, 128), (0, 1, 3, 2, 4)).reshape(512, 2, 2, 1024)

    return jax.shard_map(
        local_apply,
        mesh=mesh,
        in_specs=(P("bx", None, None, "by"), P("bx", None, None), P(), P("by", None, None)),
        out_specs=P("bx", None, None, "by"),
        check_vma=False,
    )
```
